32 devices in a mesh: row: 4 (over x, core), col: 8 (over z, y).
Axes of the slice: x: 2, y: 2, z: 4, core: 2. Of those that a mesh axis runs over, the one named last changes fastest.
Arguments:
- x_rows: float32 [16, 16384], P(None, ('row', 'col')), may hold values from -6 to 6
- alpha_rows: float32 [16384], P(('row', 'col')), may hold values from -0.5 to 1.5
- x_cols: float32 [16, 8192], P(None, ('col', 'row')), may hold values from -6 to 6
- alpha_cols: float32 [8192], P(('col', 'row')), may hold values from -0.0073242188 to 0.021972656
- lengthscale: float32 [16], replicated, may hold values from 1.2 to 2.5
Outputs:
- row_terms: float32 [16, 16384], P(None, ('row', 'col'))
- kernel_alpha: float32 [16384], P(('row', 'col'))
- grad: float32 [16], replicated
The draws below stay inside these ranges and needn't reach their ends.
All inputs are finite; a program needn't handle non-finite values.
Results may differ from the reference program's by a relative error of at most 0.00021.
Values sent between devices are 32-bit elements; how exact they have to be, the bound alone decides.
A program may use at most 64 MiB of HBM per device.

```python
import math
import jax
import jax.numpy as jnp
from jax import lax

DIMS = 16
ROWS = 16384
NPTS = 8192


def block_levels(rng, shape, split, low, high):
    gain = 1.0
    for position, parts in split:
        draws = jax.random.uniform(jax.random.fold_in(jax.random.fold_in(rng, 6), position), (parts,), jnp.float32, low / len(split), high / len(split))
        gain = gain * jnp.repeat(jnp.exp(draws), shape[position] // parts).reshape((-1,) + (1,) * (len(shape) - 1 - position))
    return gain


def bell_draw(stream_key, extent, spread, most, shards=(), kind=jnp.bfloat16):
    entries = jax.random.normal(stream_key, extent, jnp.float32) * spread
    if len(shards) > 0:
        entries = block_levels(stream_key, extent, shards, -0.22, 0.18) * entries
    return jnp.clip(entries, min=-most, max=most).astype(kind)


def setup_inputs(seed: int = 0) -> dict:
    seeds = jax.random.split(jax.random.key(seed), 6)
    return {
        "x_rows": bell_draw(seeds[0], (DIMS, ROWS), 1.0, 6.0, ((1, 32),), jnp.float32),
        "alpha_rows": jnp.clip(-0.5 + 2.0 * jax.random.uniform(seeds[1], (ROWS,), jnp.float32) ** block_levels(seeds[1], (ROWS,), ((0, 32),), -0.2, 0.2), -0.5, 1.5),
        "x_cols": bell_draw(seeds[2], (DIMS, NPTS), 1.0, 6.0, ((1, 32),), jnp.float32),
        "alpha_cols": jnp.clip(-0.0073242188 + 0.029296875 * jax.random.uniform(seeds[3], (NPTS,), jnp.float32) ** block_levels(seeds[3], (NPTS,), ((0, 32),), -0.2, 0.2), -0.0073242188, 0.021972656),
        "lengthscale": jnp.clip(jnp.exp(jax.random.uniform(seeds[4], (DIMS,), jnp.float32, math.log(1.2), math.log(2.5))), 1.2, 2.5),
    }


def fold_terms(partials, row_scaled, row_alpha):
    dims = row_scaled.shape[0]
    weight_sum = partials[0]
    first_moment = partials[1:1 + dims]
    second_moment = partials[1 + dims:]
    terms = 0.5 * row_alpha[None, :] * (row_scaled * row_scaled * weight_sum[None, :] - 2.0 * row_scaled * first_moment + second_moment)
    return terms, weight_sum


def reference(x_rows, alpha_rows, x_cols, alpha_cols, lengthscale):
    inverse_scale = 1.0 / lengthscale
    row_scaled = x_rows * inverse_scale[:, None]
    col_scaled = x_cols * inverse_scale[:, None]
    col_norms = jnp.sum(col_scaled * col_scaled, 0)
    values = jnp.concatenate([alpha_cols[None, :], alpha_cols[None, :] * col_scaled, alpha_cols[None, :] * col_scaled * col_scaled], 0)
    block_rows = min(512, ROWS)
    block_count = ROWS // block_rows
    blocks = jnp.transpose(row_scaled.reshape(DIMS, block_count, block_rows), (1, 0, 2))

    def one_block(row_block):
        row_norms = jnp.sum(row_block * row_block, 0)
        cross = lax.dot_general(row_block, col_scaled, (((0,), (0,)), ((), ())), precision=lax.Precision.HIGHEST, preferred_element_type=jnp.float32)
        kernel = jnp.exp(-0.5 * (row_norms[:, None] + col_norms[None, :] - 2.0 * cross))
        return lax.dot_general(values, kernel, (((1,), (1,)), ((), ())), precision=lax.Precision.HIGHEST, preferred_element_type=jnp.float32)

    pieces = lax.map(one_block, blocks)
    partials = jnp.transpose(pieces, (1, 0, 2)).reshape(2 * DIMS + 1, ROWS)
    terms, weight_sum = fold_terms(partials, row_scaled, alpha_rows)
    grad = jnp.sum(terms, 1) / ROWS
    return terms, weight_sum, grad
```

```python
import functools

import jax
import jax.numpy as jnp
from jax import lax
from jax.experimental import pallas as pl
from jax.experimental.pallas import tpu as pltpu
from jax.sharding import PartitionSpec as P

LOG2E = 1.4426950408889634
CORES = 2
MESH = pl.DeviceIdType.MESH
F32 = jnp.float32
BF16 = jnp.bfloat16
scope = jax.named_scope


def split3(value):
    high = value.astype(BF16)
    rest = value - high.astype(F32)
    mid = rest.astype(BF16)
    low = (rest - mid.astype(F32)).astype(BF16)
    return high, mid, low


def split2(value):
    high = value.astype(BF16)
    mid = (value - high.astype(F32)).astype(BF16)
    return high, mid


def stack_rows(count, rows):
    index = lax.broadcasted_iota(jnp.int32, (16, count), 0)
    out = jnp.zeros((16, count), F32)
    for place, row in enumerate(rows):
        row = row.astype(F32) if hasattr(row, "astype") else row
        out = jnp.where(index == place, row, out)
    return out.astype(BF16)


def layout(row_size, col_size):
    n_x = row_size // CORES
    n_y = n_x if col_size % n_x == 0 else 1
    return n_x, n_y, col_size // n_y


def far_first(row_size, col_size):
    n_x, n_y, n_z = layout(row_size, col_size)
    steps = [
        (dx, core, dz, dy)
        for dx in range(n_x)
        for core in range(CORES)
        for dz in range(n_z)
        for dy in range(n_y)
    ]
    steps.remove((0, 0, 0, 0))

    def hops(step):
        dx, core, dz, dy = step
        return min(dx, n_x - dx) + min(dy, n_y - dy) + min(dz, n_z - dz), core

    return sorted(steps, key=hops, reverse=True)


def kernel(
    row_size,
    col_size,
    xr_hbm,
    ar_hbm,
    xc_hbm,
    ac_hbm,
    ls_hbm,
    terms_ref,
    sums_ref,
    grad_ref,
    ls_ref,
    rows,
    cols,
    row_aug,
    acc,
    shares,
    incoming,
    part,
    parts,
    local,
    ready,
    send_r,
    recv_r,
    send_y,
    recv_y,
    send_n,
    recv_n,
    send_f,
    recv_f,
    send_t,
    recv_t,
    send_g,
    recv_g,
):
    n_rows, wide, row_count = rows.shape
    dims = wide - 1
    col_count = cols.shape[3]
    n_x, n_y, n_z = layout(row_size, col_size)
    n_all = row_size * col_size
    my_row = lax.axis_index("row")
    my_col = lax.axis_index("col")
    my_x, my_core = my_row // CORES, my_row % CORES
    my_z, my_y = my_col // n_y, my_col % n_y

    def row_peer(k):
        return (
            (my_x + k // CORES) % n_x * CORES + (my_core + k % CORES) % CORES,
            my_col,
        )

    def back(k):
        return (n_x - k // CORES) % n_x * CORES + k % CORES

    def y_peer(m):
        return (my_row, my_z * n_y + (my_y + m) % n_y)

    def z_peer(z):
        return (my_row, z * n_y + my_y)

    above, below = my_z < n_z - 1, my_z > 0
    sides = ((1, above), (-1, below))

    barrier = pltpu.get_barrier_semaphore()
    for sign, there in sides:

        @pl.when(there)
        def _():
            pl.semaphore_signal(
                barrier, inc=1, device_id=z_peer(my_z + sign), device_id_type=MESH
            )

    for m in range(1, n_y):
        pl.semaphore_signal(barrier, inc=1, device_id=y_peer(m), device_id_type=MESH)
    for k in range(row_size - 1, 0, -1):
        pl.semaphore_signal(barrier, inc=1, device_id=row_peer(k), device_id_type=MESH)

    loads = [
        pltpu.make_async_copy(xc_hbm, cols.at[my_z, 0, pl.ds(0, dims)], local.at[0]),
        pltpu.make_async_copy(ac_hbm, cols.at[my_z, 0, pl.ds(dims, 1)], local.at[1]),
        pltpu.make_async_copy(xr_hbm, rows.at[0, pl.ds(0, dims)], local.at[2]),
        pltpu.make_async_copy(ar_hbm, rows.at[0, pl.ds(dims, 1)], local.at[3]),
        pltpu.make_async_copy(ls_hbm, ls_ref, local.at[4]),
    ]
    for copy in loads:
        copy.start()

    def remote(src, dst, send, recv, peer):
        return pltpu.make_async_remote_copy(src, dst, send, recv, peer, MESH)

    def row_copy(k):
        return remote(
            rows.at[0], rows.at[back(k)], send_r.at[k], recv_r.at[back(k)], row_peer(k)
        )

    def row_arrival(k):
        return remote(rows.at[0], rows.at[k], send_r.at[k], recv_r.at[k], row_peer(k))

    def y_copy(m):
        at = n_y - m
        return remote(
            cols.at[my_z, 0], cols.at[my_z, at], send_y.at[m], recv_y.at[at], y_peer(m)
        )

    def y_arrival(m):
        return remote(
            cols.at[my_z, 0], cols.at[my_z, m], send_y.at[m], recv_y.at[m], y_peer(m)
        )

    def near_copy(sign, m):
        return remote(
            cols.at[my_z, m],
            cols.at[my_z, m],
            send_n.at[(sign + 1) // 2, m],
            recv_n.at[my_z, m],
            z_peer(my_z + sign),
        )

    def near_arrival(z, m):
        return remote(
            cols.at[z, m], cols.at[z, m], send_n.at[0, m], recv_n.at[z, m], z_peer(z)
        )

    def far_copy(z):
        return remote(cols.at[my_z], cols.at[my_z], send_f.at[z], recv_f.at[my_z], z_peer(z))

    def far_arrival(z):
        return remote(cols.at[z], cols.at[z], send_f.at[z], recv_f.at[z], z_peer(z))

    def term_copy(k):
        return remote(
            shares.at[k], incoming.at[back(k)], send_t.at[k], recv_t.at[back(k)], row_peer(k)
        )

    def term_arrival(k):
        return remote(shares.at[k], incoming.at[k], send_t.at[k], recv_t.at[k], row_peer(k))

    steps = far_first(row_size, col_size)

    def g_copy(place):
        dx, core, dz, dy = steps[place]
        peer = (
            (my_x + dx) % n_x * CORES + (my_core + core) % CORES,
            (my_z + dz) % n_z * n_y + (my_y + dy) % n_y,
        )
        return remote(
            part.at[pl.ds(0, 1)], parts.at[place], send_g.at[place], recv_g.at[place], peer
        )

    with scope("load"):
        for copy in loads:
            copy.wait()

    eye = lax.broadcasted_iota(jnp.int32, (dims, dims), 0) == lax.broadcasted_iota(
        jnp.int32, (dims, dims), 1
    )
    scale = jnp.sum(jnp.where(eye, jnp.broadcast_to(ls_ref[...], (dims, dims)), 0.0), 1, keepdims=True)
    inverse = 1.0 / scale

    def prepare_rows(k):
        row_scaled = rows[k, 0:dims] * inverse
        row_norm = (-0.5 * LOG2E) * jnp.sum(row_scaled * row_scaled, 0, keepdims=True)
        rh, rm, rl = split3(row_scaled * LOG2E)
        row_aug[k] = jnp.concatenate(
            [rh, rh, rh, rm, rm, rl, stack_rows(row_count, (1.0, 1.0, 1.0) + split3(row_norm))], 0
        )

    def operands(z, m):
        x, alpha = cols[z, m, 0:dims], cols[z, m, dims : dims + 1]
        scaled = x * inverse
        norm = (-0.5 * LOG2E) * jnp.sum(scaled * scaled, 0, keepdims=True)
        ch, cm, cl = split3(scaled)
        col_aug = jnp.concatenate(
            [ch, cm, cl, ch, cm, ch, stack_rows(col_count, split3(norm) + (1.0, 1.0, 1.0))], 0
        )
        first = alpha * scaled
        fh, fm = split2(first)
        sh, sm = split2(first * scaled)
        left = jnp.concatenate([fh, sh, fm, sm, stack_rows(col_count, split3(alpha))], 0)
        return col_aug, left

    def contribute(chunks, blocks, fresh=False):
        made = [operands(z, m) for z, m in chunks]
        steps = [(k, at) for k in blocks for at in range(len(chunks))]
        exponents, values = {}, {}
        for now in range(len(steps) + 2):
            if now < len(steps):
                k, at = steps[now]
                exponents[now] = lax.dot_general(
                    made[at][0], row_aug[k], (((0,), (0,)), ((), ())), preferred_element_type=F32
                )
            if now >= 2:
                k, at = steps[now - 2]
                left = made[at][1]
                more = jnp.dot(
                    jnp.concatenate([left, left], 1),
                    jnp.concatenate(values.pop(now - 2), 0),
                    preferred_element_type=F32,
                )
                if fresh and at == 0:
                    acc[k] = more
                else:
                    acc[k] += more
            if 1 <= now <= len(steps):
                values[now - 1] = split2(jnp.exp2(exponents.pop(now - 1)))

    prepare_rows(0)

    with scope("bar"):
        pl.semaphore_wait(barrier, row_size + n_y - 2 + sum(there.astype(jnp.int32) for _, there in sides))

    with scope("near"):
        @pl.when(jnp.logical_and(above, below))
        def _():
            for sign in (1, -1):
                pl.semaphore_signal(
                    ready.at[my_z + sign],
                    inc=1,
                    device_id=z_peer(my_z - sign),
                    device_id_type=MESH,
                )

        for m in range(1, n_y):
            y_copy(m).start()
        for sign, there in sides:

            @pl.when(there)
            def _():
                near_copy(sign, 0).start()

        for k in list(range(CORES, row_size)) + [1]:
            row_copy(k).start()

    with scope("c00"):
        contribute([(my_z, 0)], [0], fresh=True)

    def learn(d):
        for sign, there in sides:
            opposite = my_z - sign
            z = my_z + sign * d
            inside = jnp.logical_and(z >= 0, z < n_z)

            @pl.when(inside)
            def _():
                pl.semaphore_wait(ready.at[z], 1)

            @pl.when(jnp.logical_and(inside, jnp.logical_and(opposite >= 0, opposite < n_z)))
            def _():
                pl.semaphore_signal(
                    ready.at[z], inc=1, device_id=z_peer(opposite), device_id_type=MESH
                )

    def send_far(d):
        for sign, _ in sides:
            z = my_z + sign * d

            @pl.when(jnp.logical_and(z >= 0, z < n_z))
            def _():
                far_copy(z).start()

    if n_z > 2:
        with scope("rdy2"):
            learn(2)

    with scope("c01"):
        row_arrival(1).wait_recv()
        prepare_rows(1)
        contribute([(my_z, 0)], [1], fresh=True)

    with scope("ywait"):
        for m in range(1, n_y):
            y_arrival(m).wait_recv()

    with scope("fsend"):
        if n_z > 2:
            send_far(2)
        for sign, there in sides:

            @pl.when(there)
            def _():
                for m in range(1, n_y):
                    near_copy(sign, m).start()

    with scope("cy"):
        contribute([(my_z, m) for m in range(1, n_y)], [0, 1])

    with scope("rdy3"):
        for d in range(3, n_z):
            learn(d)
            send_far(d)

    with scope("roww"):
        for k in range(CORES, row_size):
            row_arrival(k).wait_recv()
    with scope("crow"):
        for k in range(CORES, row_size):
            prepare_rows(k)
        contribute([(my_z, m) for m in range(n_y)], range(CORES, row_size), fresh=True)

    low = jnp.minimum(my_z, n_z - 1 - my_z)
    far_sign = jnp.where(2 * my_z < n_z - 1, 1, -1)
    for t in range(1, n_z):
        near_z = my_z + (1 if t % 2 else -1) * ((t + 1) // 2)
        z = jnp.where(t <= 2 * low, near_z, my_z + far_sign * (t - low))
        is_near = jnp.logical_or(z == my_z + 1, z == my_z - 1)
        with scope("zw"):

            @pl.when(is_near)
            def _():
                for m in range(n_y):
                    near_arrival(z, m).wait_recv()

            @pl.when(jnp.logical_not(is_near))
            def _():
                far_arrival(z).wait_recv()

        with scope("cz"):
            contribute([(z, m) for m in range(n_y)], range(row_size))

    with scope("fold"):
        folded = None
        for k in range(row_size):
            total = acc[k]
            row_scaled = rows[k, 0:dims] * inverse
            first = total[0:16] + total[32:48]
            second = total[16:32] + total[48:64]
            weight = total[64:65] + total[65:66] + total[66:67]
            share = (0.5 * rows[k, dims : dims + 1]) * (
                row_scaled * row_scaled * weight - 2.0 * row_scaled * first + second
            )
            shares[k, 0:dims] = share
            shares[k, dims : dims + 1] = weight
            for at in range(0, row_count, 128):
                piece = share[:, at : at + 128]
                folded = piece if folded is None else folded + piece
        gathered = lax.dot_general(
            jnp.ones((8, 128), F32),
            folded,
            (((1,), (1,)), ((), ())),
            precision=lax.Precision.HIGHEST,
            preferred_element_type=F32,
        )
        part[...] = jnp.zeros_like(part)
        part[:, 0:dims] = gathered

    with scope("gst"):
        for place in range(n_all - 1):
            g_copy(place).start()
        for k in list(range(CORES, row_size)) + [1]:
            term_copy(k).start()

    with scope("drain"):
        for m in range(1, n_y):
            y_copy(m).wait_send()
        for k in range(1, row_size):
            row_copy(k).wait_send()
        for sign, there in sides:

            @pl.when(there)
            def _():
                for m in range(n_y):
                    near_copy(sign, m).wait_send()

            for d in range(2, n_z):
                z = my_z + sign * d

                @pl.when(jnp.logical_and(z >= 0, z < n_z))
                def _():
                    far_copy(z).wait_send()

    with scope("twait"):
        for k in range(1, row_size):
            term_arrival(k).wait_recv()
    with scope("tsum"):
        whole = shares[0]
        for k in range(1, row_size):
            whole = whole + incoming[k]
        terms_ref[...] = whole[0:dims]
        sums_ref[...] = whole[dims : dims + 1]
        parts[n_all - 1] = part[0:1]
    with scope("gwait"):
        for place in range(n_all - 1):
            g_copy(place).wait()
    with scope("gsum"):
        grad_ref[...] = (jnp.sum(parts[...], 0) / (row_count * n_all))[:, 0:dims]
        for k in range(1, row_size):
            term_copy(k).wait_send()


def settle(terms_in, sums_in, grad_in, terms_out, sums_out, grad_out, sems):
    copies = [
        pltpu.make_async_copy(terms_in, terms_out, sems.at[0]),
        pltpu.make_async_copy(sums_in, sums_out, sems.at[1]),
        pltpu.make_async_copy(grad_in, grad_out, sems.at[2]),
    ]
    for copy in copies:
        copy.start()
    for copy in copies:
        copy.wait()


def on_device(row_size, col_size, x_rows, alpha_rows, x_cols, alpha_cols, lengthscale):
    dims, row_count = x_rows.shape
    col_count = x_cols.shape[1]
    _, n_y, n_z = layout(row_size, col_size)
    n_all = row_size * col_size
    vmem = pl.BlockSpec(memory_space=pltpu.VMEM)
    anywhere = pl.BlockSpec(memory_space=pl.ANY)
    dma = pltpu.SemaphoreType.DMA
    terms, sums, grad = pl.pallas_call(
        functools.partial(kernel, row_size, col_size),
        out_shape=(
            pltpu.VMEM((dims, row_count), F32),
            pltpu.VMEM((1, row_count), F32),
            pltpu.VMEM((1, dims), F32),
        ),
        in_specs=[pl.BlockSpec(memory_space=pltpu.HBM)] * 5,
        out_specs=(vmem, vmem, vmem),
        scratch_shapes=[
            pltpu.VMEM((1, dims), F32),
            pltpu.VMEM((row_size, dims + 1, row_count), F32),
            pltpu.VMEM((n_z, n_y, dims + 1, col_count), F32),
            pltpu.VMEM((row_size, 112, row_count), BF16),
            pltpu.VMEM((row_size, 80, row_count), F32),
            pltpu.VMEM((row_size, dims + 1, row_count), F32),
            pltpu.VMEM((row_size, dims + 1, row_count), F32),
            pltpu.VMEM((8, 128), F32),
            pltpu.VMEM((n_all, 1, 128), F32),
            dma((5,)),
            pltpu.SemaphoreType.REGULAR((n_z,)),
            dma((row_size,)),
            dma((row_size,)),
            dma((n_y,)),
            dma((n_y,)),
            dma((2, n_y)),
            dma((n_z, n_y)),
            dma((n_z,)),
            dma((n_z,)),
            dma((row_size,)),
            dma((row_size,)),
            dma((n_all,)),
            dma((n_all,)),
        ],
        compiler_params=pltpu.CompilerParams(
            collective_id=0, has_side_effects=True
        ),
    )(
        x_rows,
        alpha_rows.reshape(1, row_count),
        x_cols,
        alpha_cols.reshape(1, col_count),
        lengthscale.reshape(1, dims),
    )
    terms, sums, grad = pl.pallas_call(
        settle,
        out_shape=[jax.ShapeDtypeStruct(x.shape, x.dtype) for x in (terms, sums, grad)],
        in_specs=[vmem] * 3,
        out_specs=(anywhere, anywhere, anywhere),
        scratch_shapes=[dma((3,))],
        compiler_params=pltpu.CompilerParams(vmem_limit_bytes=16 * 1024 * 1024),
    )(terms, sums, grad)
    return terms, sums.reshape(row_count), grad.reshape(dims)


def solution(mesh):
    return jax.shard_map(
        functools.partial(on_device, mesh.shape["row"], mesh.shape["col"]),
        mesh=mesh,
        in_specs=(
            P(None, ("row", "col")),
            P(("row", "col")),
            P(None, ("col", "row")),
            P(("col", "row")),
            P(),
        ),
        out_specs=(P(None, ("row", "col")), P(("row", "col")), P()),
        check_vma=False,
    )
```

```python
import functools

import jax
import jax.numpy as jnp
from jax import lax
from jax.experimental import pallas as pl
from jax.experimental.pallas import tpu as pltpu
from jax.sharding import PartitionSpec as P

LOG2E = 1.4426950408889634
CORES = 2
MESH = pl.DeviceIdType.MESH
F32 = jnp.float32
BF16 = jnp.bfloat16
scope = jax.named_scope
LAG = 2


def split3(value):
    high = value.astype(BF16)
    rest = value - high.astype(F32)
    mid = rest.astype(BF16)
    low = (rest - mid.astype(F32)).astype(BF16)
    return high, mid, low


def split2(value):
    high = value.astype(BF16)
    mid = (value - high.astype(F32)).astype(BF16)
    return high, mid


def stack_rows(count, rows):
    index = lax.broadcasted_iota(jnp.int32, (16, count), 0)
    out = jnp.zeros((16, count), F32)
    for place, row in enumerate(rows):
        row = row.astype(F32) if hasattr(row, "astype") else row
        out = jnp.where(index == place, row, out)
    return out.astype(BF16)


def layout(row_size, col_size):
    n_x = row_size // CORES
    n_y = n_x if col_size % n_x == 0 else 1
    return n_x, n_y, col_size // n_y


def far_first(row_size, col_size):
    n_x, n_y, n_z = layout(row_size, col_size)
    steps = [
        (dx, core, dz, dy)
        for dx in range(n_x)
        for core in range(CORES)
        for dz in range(n_z)
        for dy in range(n_y)
    ]
    steps.remove((0, 0, 0, 0))

    def hops(step):
        dx, core, dz, dy = step
        return min(dx, n_x - dx) + min(dy, n_y - dy) + min(dz, n_z - dz), core

    return sorted(steps, key=hops, reverse=True)


def kernel(
    row_size,
    col_size,
    xr_hbm,
    ar_hbm,
    xc_hbm,
    ac_hbm,
    ls_hbm,
    terms_ref,
    sums_ref,
    grad_ref,
    ls_ref,
    rows,
    row_alpha,
    cols,
    col_alpha,
    row_aug,
    acc,
    values,
    lefts,
    shares,
    share_sums,
    incoming,
    incoming_sums,
    part,
    parts,
    local,
    sent,
    recv_r,
    recv_ra,
    recv_c,
    recv_t,
    recv_g,
):
    _, dims, row_count = rows.shape
    col_count = cols.shape[2]
    n_x, n_y, n_z = layout(row_size, col_size)
    n_all = row_size * col_size
    my_row = lax.axis_index("row")
    my_col = lax.axis_index("col")
    my_x, my_core = my_row // CORES, my_row % CORES
    my_z, my_y = my_col // n_y, my_col % n_y

    def row_peer(k):
        return (
            (my_x + k // CORES) % n_x * CORES + (my_core + k % CORES) % CORES,
            my_col,
        )

    def back(k):
        return (n_x - k // CORES) % n_x * CORES + k % CORES

    low = jnp.minimum(my_z, n_z - 1 - my_z)
    far_sign = jnp.where(2 * my_z < n_z - 1, 1, -1)
    order = [my_z]
    for t in range(1, n_z):
        near = my_z + (1 if t % 2 else -1) * ((t + 1) // 2)
        order.append(jnp.where(t <= 2 * low, near, my_z + far_sign * (t - low)))
    places = [
        [z * n_y + (my_y + m) % n_y for m in range(n_y)] for z in order
    ]
    ordered = [c for line in places for c in line]
    col_peers = ordered[1:]
    row_steps = list(range(CORES, row_size)) + [1]

    barrier = pltpu.get_barrier_semaphore()
    for c in reversed(col_peers):
        pl.semaphore_signal(barrier, inc=1, device_id=(my_row, c), device_id_type=MESH)
    for k in row_steps:
        pl.semaphore_signal(barrier, inc=1, device_id=row_peer(k), device_id_type=MESH)

    loads = [
        pltpu.make_async_copy(xc_hbm, cols.at[my_col], local.at[0]),
        pltpu.make_async_copy(ac_hbm, col_alpha.at[my_col], local.at[1]),
        pltpu.make_async_copy(xr_hbm, rows.at[0], local.at[2]),
        pltpu.make_async_copy(ar_hbm, row_alpha.at[0], local.at[3]),
        pltpu.make_async_copy(ls_hbm, ls_ref, local.at[4]),
    ]
    for copy in loads:
        copy.start()

    def remote(src, dst, send, recv, peer):
        return pltpu.make_async_remote_copy(src, dst, send, recv, peer, MESH)

    def row_copy(k, which):
        ref, there = (rows, row_alpha)[which], back(k)
        return remote(
            ref.at[0],
            ref.at[there],
            sent.at[which],
            recv_ra.at[0] if which else recv_r.at[there],
            row_peer(k),
        )

    def bytes_of(ref, count, send, recv):
        return remote(ref.at[pl.ds(0, count)], ref.at[pl.ds(0, count)], send, recv, row_peer(1))

    def row_arrival(k):
        return remote(rows.at[0], rows.at[k], sent.at[0], recv_r.at[k], row_peer(k))

    def col_copy(c, which):
        ref = (cols, col_alpha)[which]
        return remote(
            ref.at[my_col], ref.at[my_col], sent.at[2 + which], recv_c.at[which, my_z], (my_row, c)
        )

    def term_copy(k, which):
        src, dst = ((shares, incoming), (share_sums, incoming_sums))[which]
        there = back(k)
        return remote(
            src.at[k], dst.at[there], sent.at[4 + which], recv_t.at[which], row_peer(k)
        )

    steps = far_first(row_size, col_size)

    def g_copy(place):
        dx, core, dz, dy = steps[place]
        peer = (
            (my_x + dx) % n_x * CORES + (my_core + core) % CORES,
            (my_z + dz) % n_z * n_y + (my_y + dy) % n_y,
        )
        return remote(
            part.at[pl.ds(0, 1)], parts.at[place], sent.at[6], recv_g.at[0], peer
        )

    with scope("load"):
        for copy in loads:
            copy.wait()

    eye = lax.broadcasted_iota(jnp.int32, (dims, dims), 0) == lax.broadcasted_iota(
        jnp.int32, (dims, dims), 1
    )
    scale = jnp.sum(jnp.where(eye, jnp.broadcast_to(ls_ref[...], (dims, dims)), 0.0), 1, keepdims=True)
    inverse = 1.0 / scale

    def prepare_rows(k):
        row_scaled = rows[k] * inverse
        row_norm = (-0.5 * LOG2E) * jnp.sum(row_scaled * row_scaled, 0, keepdims=True)
        rh, rm, rl = split3(row_scaled * LOG2E)
        row_aug[k] = jnp.concatenate(
            [rh, rh, rh, rm, rm, rl, stack_rows(row_count, (1.0, 1.0, 1.0) + split3(row_norm))], 0
        )

    def operands(c):
        x, alpha = cols[c], col_alpha[c]
        scaled = x * inverse
        norm = (-0.5 * LOG2E) * jnp.sum(scaled * scaled, 0, keepdims=True)
        ch, cm, cl = split3(scaled)
        col_aug = jnp.concatenate(
            [ch, cm, cl, ch, cm, ch, stack_rows(col_count, split3(norm) + (1.0, 1.0, 1.0))], 0
        )
        first = alpha * scaled
        fh, fm = split2(first)
        sh, sm = split2(first * scaled)
        group = stack_rows(col_count, split3(alpha))
        left = jnp.concatenate([fh, sh, fm, sm, group] + [jnp.zeros_like(group)] * 3, 0)
        return col_aug, left

    waiting, begun, made = [], set(), {}
    slots = values.shape[0]
    count = 0

    def add_up():
        k, place, slot = waiting.pop(0)
        left = lefts[place]
        more = jnp.dot(
            jnp.concatenate([left, left], 1), values[slot], preferred_element_type=F32
        )
        more = more[0:80]
        if k in begun:
            acc[k] += more
        else:
            acc[k] = more
        begun.add(k)

    def contribute(pairs, last=False):
        nonlocal count
        pairs = list(pairs)
        while waiting:
            add_up()
        augs, exponents = {}, {}

        def settle_values(now):
            nonlocal count
            high, mid = split2(jnp.exp2(exponents.pop(now)))
            slot = count % slots
            count += 1
            values[slot, 0:col_count] = high
            values[slot, col_count : 2 * col_count] = mid
            waiting.append((pairs[now][1], pairs[now][0], slot))

        for now, (place, k) in enumerate(pairs):
            if place not in augs:
                augs[place], left = operands(ordered[place])
                if place not in made:
                    lefts[place] = left
                    made[place] = True
            exponents[now] = lax.dot_general(
                augs[place], row_aug[k], (((0,), (0,)), ((), ())), preferred_element_type=F32
            )
            if len(waiting) >= LAG - 1:
                add_up()
            if now:
                settle_values(now - 1)
        while waiting:
            add_up()
        settle_values(len(pairs) - 1)
        while last and waiting:
            add_up()

    prepare_rows(0)

    with scope("bar"):
        pl.semaphore_wait(barrier, row_size + col_size - 2)

    with scope("send"):
        for k in row_steps:
            row_copy(k, 0).start()
        for c in col_peers:
            col_copy(c, 0).start()
            col_copy(c, 1).start()
        for k in row_steps:
            row_copy(k, 1).start()

    with scope("c00"):
        contribute([(0, 0)], last=True)

    with scope("w01"):
        row_arrival(1).wait_recv()
    with scope("c01"):
        prepare_rows(1)
        contribute([(0, 1)], last=True)

    def arrive(z, chunks):
        for which, ref in enumerate((cols, col_alpha)):
            bytes_of(ref, chunks, sent.at[2 + which], recv_c.at[which, z]).wait_recv()

    with scope("wrow"):
        for k in range(CORES, row_size):
            row_arrival(k).wait_recv()
        if n_y > 1:
            arrive(my_z, n_y - 1)
    with scope("crow"):
        for k in range(CORES, row_size):
            prepare_rows(k)
        contribute(
            [(0, k) for k in range(CORES, row_size)]
            + [(m, k) for m in range(1, n_y) for k in range(row_size)]
        )

    for at in range(1, n_z):
        with scope("wz"):
            arrive(order[at], n_y)
        with scope("cz"):
            contribute(
                [(at * n_y + m, k) for m in range(n_y) for k in range(row_size)],
                last=at == n_z - 1,
            )

    with scope("fold"):
        bytes_of(row_alpha, row_size - 1, sent.at[1], recv_ra.at[0]).wait_recv()
        folded = None
        for k in range(row_size):
            total = acc[k]
            row_scaled = rows[k] * inverse
            first = total[0:16] + total[32:48]
            second = total[16:32] + total[48:64]
            weight = total[64:65] + total[65:66] + total[66:67]
            share = (0.5 * row_alpha[k]) * (
                row_scaled * row_scaled * weight - 2.0 * row_scaled * first + second
            )
            shares[k] = share
            share_sums[k] = weight
            for at in range(0, row_count, 128):
                piece = share[:, at : at + 128]
                folded = piece if folded is None else folded + piece
        gathered = lax.dot_general(
            jnp.ones((8, 128), F32),
            folded,
            (((1,), (1,)), ((), ())),
            precision=lax.Precision.HIGHEST,
            preferred_element_type=F32,
        )
        part[...] = jnp.zeros_like(part)
        part[:, 0:dims] = gathered

    with scope("gst"):
        for place in range(n_all - 1):
            g_copy(place).start()
        for k in row_steps:
            for which in (0, 1):
                term_copy(k, which).start()

    with scope("drain"):
        for which, ref in enumerate((rows, row_alpha)):
            bytes_of(ref, row_size - 1, sent.at[which], recv_r.at[0]).wait_send()
        for which, ref in enumerate((cols, col_alpha)):
            bytes_of(ref, col_size - 1, sent.at[2 + which], recv_r.at[0]).wait_send()

    with scope("twait"):
        for which, ref in enumerate((incoming, incoming_sums)):
            bytes_of(ref, row_size - 1, sent.at[4 + which], recv_t.at[which]).wait_recv()
    with scope("tsum"):
        terms, sums = shares[0], share_sums[0]
        for k in range(1, row_size):
            terms = terms + incoming[k]
            sums = sums + incoming_sums[k]
        terms_ref[...] = terms
        sums_ref[...] = sums
        parts[n_all - 1] = part[0:1]
    with scope("gwait"):
        bytes_of(parts, n_all - 1, sent.at[6], recv_g.at[0]).wait()
    with scope("gsum"):
        grad_ref[...] = (jnp.sum(parts[...], 0) / (row_count * n_all))[:, 0:dims]
        for which, ref in enumerate((shares, share_sums)):
            bytes_of(ref, row_size - 1, sent.at[4 + which], recv_t.at[which]).wait_send()


def settle(terms_in, sums_in, grad_in, terms_out, sums_out, grad_out, sems):
    copies = [
        pltpu.make_async_copy(terms_in, terms_out, sems.at[0]),
        pltpu.make_async_copy(sums_in, sums_out, sems.at[1]),
        pltpu.make_async_copy(grad_in, grad_out, sems.at[2]),
    ]
    for copy in copies:
        copy.start()
    for copy in copies:
        copy.wait()


def on_device(row_size, col_size, x_rows, alpha_rows, x_cols, alpha_cols, lengthscale):
    dims, row_count = x_rows.shape
    col_count = x_cols.shape[1]
    _, _, n_z = layout(row_size, col_size)
    n_all = row_size * col_size
    vmem = pl.BlockSpec(memory_space=pltpu.VMEM)
    anywhere = pl.BlockSpec(memory_space=pl.ANY)
    dma = pltpu.SemaphoreType.DMA
    terms, sums, grad = pl.pallas_call(
        functools.partial(kernel, row_size, col_size),
        out_shape=(
            pltpu.VMEM((dims, row_count), F32),
            pltpu.VMEM((1, row_count), F32),
            pltpu.VMEM((1, dims), F32),
        ),
        in_specs=[pl.BlockSpec(memory_space=pltpu.HBM)] * 5,
        out_specs=(vmem, vmem, vmem),
        scratch_shapes=[
            pltpu.VMEM((1, dims), F32),
            pltpu.VMEM((row_size, dims, row_count), F32),
            pltpu.VMEM((row_size, 1, row_count), F32),
            pltpu.VMEM((col_size, dims, col_count), F32),
            pltpu.VMEM((col_size, 1, col_count), F32),
            pltpu.VMEM((row_size, 112, row_count), BF16),
            pltpu.VMEM((row_size, 80, row_count), F32),
            pltpu.VMEM((LAG + 1, 2 * col_count, row_count), BF16),
            pltpu.VMEM((col_size, 128, col_count), BF16),
            pltpu.VMEM((row_size, dims, row_count), F32),
            pltpu.VMEM((row_size, 1, row_count), F32),
            pltpu.VMEM((row_size, dims, row_count), F32),
            pltpu.VMEM((row_size, 1, row_count), F32),
            pltpu.VMEM((8, 128), F32),
            pltpu.VMEM((n_all, 1, 128), F32),
            dma((5,)),
            dma((7,)),
            dma((row_size,)),
            dma((1,)),
            dma((2, n_z)),
            dma((2,)),
            dma((1,)),
        ],
        compiler_params=pltpu.CompilerParams(
            collective_id=0, has_side_effects=True
        ),
    )(
        x_rows,
        alpha_rows.reshape(1, row_count),
        x_cols,
        alpha_cols.reshape(1, col_count),
        lengthscale.reshape(1, dims),
    )
    terms, sums, grad = pl.pallas_call(
        settle,
        out_shape=[jax.ShapeDtypeStruct(x.shape, x.dtype) for x in (terms, sums, grad)],
        in_specs=[vmem] * 3,
        out_specs=(anywhere, anywhere, anywhere),
        scratch_shapes=[dma((3,))],
        compiler_params=pltpu.CompilerParams(vmem_limit_bytes=16 * 1024 * 1024),
    )(terms, sums, grad)
    return terms, sums.reshape(row_count), grad.reshape(dims)


def solution(mesh):
    return jax.shard_map(
        functools.partial(on_device, mesh.shape["row"], mesh.shape["col"]),
        mesh=mesh,
        in_specs=(
            P(None, ("row", "col")),
            P(("row", "col")),
            P(None, ("col", "row")),
            P(("col", "row")),
            P(),
        ),
        out_specs=(P(None, ("row", "col")), P(("row", "col")), P()),
        check_vma=False,
    )
```

```python
import functools

import jax
import jax.numpy as jnp
from jax import lax
from jax.experimental import pallas as pl
from jax.experimental.pallas import tpu as pltpu
from jax.sharding import PartitionSpec as P

LOG2E = 1.4426950408889634
CORES = 2
MESH = pl.DeviceIdType.MESH
F32 = jnp.float32
BF16 = jnp.bfloat16
scope = jax.named_scope
LAG = 2


def split3(value):
    high = value.astype(BF16)
    rest = value - high.astype(F32)
    mid = rest.astype(BF16)
    low = (rest - mid.astype(F32)).astype(BF16)
    return high, mid, low


def split2(value):
    high = value.astype(BF16)
    mid = (value - high.astype(F32)).astype(BF16)
    return high, mid


def stack_rows(count, rows):
    index = lax.broadcasted_iota(jnp.int32, (16, count), 0)
    out = jnp.zeros((16, count), F32)
    for place, row in enumerate(rows):
        row = row.astype(F32) if hasattr(row, "astype") else row
        out = jnp.where(index == place, row, out)
    return out.astype(BF16)


def layout(row_size, col_size):
    n_x = row_size // CORES
    n_y = n_x if col_size % n_x == 0 else 1
    return n_x, n_y, col_size // n_y


def far_first(row_size, col_size):
    n_x, n_y, n_z = layout(row_size, col_size)
    steps = [
        (dx, core, dz, dy)
        for dx in range(n_x)
        for core in range(CORES)
        for dz in range(n_z)
        for dy in range(n_y)
    ]
    steps.remove((0, 0, 0, 0))

    def hops(step):
        dx, core, dz, dy = step
        return min(dx, n_x - dx) + min(dy, n_y - dy) + min(dz, n_z - dz), core

    return sorted(steps, key=hops, reverse=True)


def kernel(
    row_size,
    col_size,
    xr_hbm,
    ar_hbm,
    xc_hbm,
    ac_hbm,
    ls_hbm,
    terms_ref,
    sums_ref,
    grad_ref,
    ls_ref,
    rows,
    row_alpha,
    cols,
    col_alpha,
    row_aug,
    acc,
    values,
    lefts,
    shares,
    share_sums,
    incoming,
    incoming_sums,
    part,
    parts,
    local,
    ready,
    sent,
    recv_r,
    recv_ra,
    recv_c,
    recv_t,
    recv_g,
):
    _, dims, row_count = rows.shape
    col_count = cols.shape[2]
    n_x, n_y, n_z = layout(row_size, col_size)
    n_all = row_size * col_size
    my_row = lax.axis_index("row")
    my_col = lax.axis_index("col")
    my_x, my_core = my_row // CORES, my_row % CORES
    my_z, my_y = my_col // n_y, my_col % n_y

    def row_peer(k):
        return (
            (my_x + k // CORES) % n_x * CORES + (my_core + k % CORES) % CORES,
            my_col,
        )

    def back(k):
        return (n_x - k // CORES) % n_x * CORES + k % CORES

    low = jnp.minimum(my_z, n_z - 1 - my_z)
    far_sign = jnp.where(2 * my_z < n_z - 1, 1, -1)
    order = [my_z]
    for t in range(1, n_z):
        near = my_z + (1 if t % 2 else -1) * ((t + 1) // 2)
        order.append(jnp.where(t <= 2 * low, near, my_z + far_sign * (t - low)))
    places = [
        [z * n_y + (my_y + m) % n_y for m in range(n_y)] for z in order
    ]
    ordered = [c for line in places for c in line]
    row_steps = list(range(CORES, row_size)) + [1]
    sides = [(1, my_z < n_z - 1), (-1, my_z > 0)]

    def line(z):
        return [(my_row, z * n_y + (my_y + m) % n_y) for m in range(n_y)]

    barrier = pltpu.get_barrier_semaphore()
    for sign, there in sides:

        @pl.when(there)
        def _():
            for peer in reversed(line(my_z + sign)):
                pl.semaphore_signal(barrier, inc=1, device_id=peer, device_id_type=MESH)

    for peer in line(my_z)[1:]:
        pl.semaphore_signal(barrier, inc=1, device_id=peer, device_id_type=MESH)
    for k in row_steps:
        pl.semaphore_signal(barrier, inc=1, device_id=row_peer(k), device_id_type=MESH)

    loads = [
        pltpu.make_async_copy(xc_hbm, cols.at[my_col], local.at[0]),
        pltpu.make_async_copy(ac_hbm, col_alpha.at[my_col], local.at[1]),
        pltpu.make_async_copy(xr_hbm, rows.at[0], local.at[2]),
        pltpu.make_async_copy(ar_hbm, row_alpha.at[0], local.at[3]),
        pltpu.make_async_copy(ls_hbm, ls_ref, local.at[4]),
    ]
    for copy in loads:
        copy.start()

    def remote(src, dst, send, recv, peer):
        return pltpu.make_async_remote_copy(src, dst, send, recv, peer, MESH)

    def row_copy(k, which):
        ref, there = (rows, row_alpha)[which], back(k)
        return remote(
            ref.at[0],
            ref.at[there],
            sent.at[which],
            recv_ra.at[0] if which else recv_r.at[there],
            row_peer(k),
        )

    def bytes_of(ref, count, send, recv):
        return remote(ref.at[pl.ds(0, count)], ref.at[pl.ds(0, count)], send, recv, row_peer(1))

    def row_arrival(k):
        return remote(rows.at[0], rows.at[k], sent.at[0], recv_r.at[k], row_peer(k))

    def col_copy(peer, which, across):
        ref = (cols, col_alpha)[which]
        return remote(
            ref.at[my_col],
            ref.at[my_col],
            sent.at[2 + which],
            recv_c.at[2 * across + which, my_z],
            peer,
        )

    def send_line(z, first=0):
        for which in (0, 1):
            for m, peer in list(enumerate(line(z)))[first:]:
                col_copy(peer, which, m > 0 and first == 0).start()

    def learn(d):
        for sign, _ in sides:
            z, other = my_z + sign * d, my_z - sign
            inside = jnp.logical_and(z >= 0, z < n_z)

            @pl.when(inside)
            def _():
                pl.semaphore_wait(ready.at[z], 1)

            @pl.when(jnp.logical_and(inside, jnp.logical_and(other >= 0, other < n_z)))
            def _():
                pl.semaphore_signal(
                    ready.at[z], inc=1, device_id=line(other)[0], device_id_type=MESH
                )

            @pl.when(inside)
            def _():
                send_line(z)

    def term_copy(k, which):
        src, dst = ((shares, incoming), (share_sums, incoming_sums))[which]
        there = back(k)
        return remote(
            src.at[k], dst.at[there], sent.at[4 + which], recv_t.at[which], row_peer(k)
        )

    steps = far_first(row_size, col_size)

    def g_copy(place):
        dx, core, dz, dy = steps[place]
        peer = (
            (my_x + dx) % n_x * CORES + (my_core + core) % CORES,
            (my_z + dz) % n_z * n_y + (my_y + dy) % n_y,
        )
        return remote(
            part.at[pl.ds(0, 1)], parts.at[place], sent.at[6], recv_g.at[0], peer
        )

    with scope("load"):
        for copy in loads:
            copy.wait()

    eye = lax.broadcasted_iota(jnp.int32, (dims, dims), 0) == lax.broadcasted_iota(
        jnp.int32, (dims, dims), 1
    )
    scale = jnp.sum(jnp.where(eye, jnp.broadcast_to(ls_ref[...], (dims, dims)), 0.0), 1, keepdims=True)
    inverse = 1.0 / scale

    def prepare_rows(k):
        row_scaled = rows[k] * inverse
        row_norm = (-0.5 * LOG2E) * jnp.sum(row_scaled * row_scaled, 0, keepdims=True)
        rh, rm, rl = split3(row_scaled * LOG2E)
        row_aug[k] = jnp.concatenate(
            [rh, rh, rh, rm, rm, rl, stack_rows(row_count, (1.0, 1.0, 1.0) + split3(row_norm))], 0
        )

    def operands(c):
        x, alpha = cols[c], col_alpha[c]
        scaled = x * inverse
        norm = (-0.5 * LOG2E) * jnp.sum(scaled * scaled, 0, keepdims=True)
        ch, cm, cl = split3(scaled)
        col_aug = jnp.concatenate(
            [ch, cm, cl, ch, cm, ch, stack_rows(col_count, split3(norm) + (1.0, 1.0, 1.0))], 0
        )
        first = alpha * scaled
        fh, fm = split2(first)
        sh, sm = split2(first * scaled)
        group = stack_rows(col_count, split3(alpha))
        left = jnp.concatenate([fh, sh, fm, sm, group], 0)
        return col_aug, left

    waiting, begun, made = [], set(), set()
    slots = values.shape[0]
    half = col_count // 2
    count = 0

    def high_sums():
        k, place, slot = waiting[0]
        return jnp.dot(lefts[place], values[slot, 0:col_count], preferred_element_type=F32)

    def mid_sums(high):
        k, place, slot = waiting.pop(0)
        left = jnp.concatenate([lefts[place, 0:32], lefts[place, 64:80]], 0)
        mid = jnp.dot(left, values[slot, col_count : 2 * col_count], preferred_element_type=F32)
        parts = (high[0:32] + mid[0:32], high[32:64], high[64:80] + mid[32:48])
        for at, more in zip((0, 32, 64), parts):
            here = slice(at, at + more.shape[0])
            if k in begun:
                acc[k, here] += more
            else:
                acc[k, here] = more
        begun.add(k)

    def exponents_of(aug, k):
        return lax.dot_general(aug, row_aug[k], (((0,), (0,)), ((), ())), preferred_element_type=F32)

    def contribute(pairs, last=False):
        nonlocal count
        pairs = list(pairs)
        while waiting:
            mid_sums(high_sums())
        augs, exponents = {}, {}

        def settle_values(now):
            nonlocal count
            slot = count % slots
            count += 1
            for at, exponent in zip((0, half), exponents.pop(now)):
                high, mid = split2(jnp.exp2(exponent))
                values[slot, at : at + half] = high
                values[slot, col_count + at : col_count + at + half] = mid
            waiting.append((pairs[now][1], pairs[now][0], slot))

        for now, (place, k) in enumerate(pairs):
            if place not in augs:
                augs[place], left = operands(ordered[place])
                if place not in made:
                    lefts[place] = left
                    made.add(place)
            near = exponents_of(augs[place][:, 0:half], k)
            high = high_sums() if waiting else None
            exponents[now] = near, exponents_of(augs[place][:, half:], k)
            if high is not None:
                mid_sums(high)
            if now:
                settle_values(now - 1)
        while waiting:
            mid_sums(high_sums())
        settle_values(len(pairs) - 1)
        while last and waiting:
            mid_sums(high_sums())

    prepare_rows(0)

    with scope("bar"):
        beside = sum(there.astype(jnp.int32) for _, there in sides)
        pl.semaphore_wait(barrier, row_size - 1 + n_y - 1 + beside * n_y)

    with scope("send"):
        @pl.when(jnp.logical_and(sides[0][1], sides[1][1]))
        def _():
            for sign in (1, -1):
                pl.semaphore_signal(
                    ready.at[my_z + sign],
                    inc=1,
                    device_id=line(my_z - sign)[0],
                    device_id_type=MESH,
                )

        send_line(my_z, 1)
        for k in row_steps:
            row_copy(k, 0).start()
        for sign, there in sides:

            @pl.when(there)
            def _():
                send_line(my_z + sign)

        for k in row_steps:
            row_copy(k, 1).start()

    with scope("c00"):
        contribute([(0, 0)], last=True)

    if n_z > 2:
        with scope("rdy2"):
            learn(2)
    with scope("w01"):
        row_arrival(1).wait_recv()
    with scope("c01"):
        prepare_rows(1)
        contribute([(0, 1)], last=True)

    def arrive(z, chunks, across=0):
        for which, ref in enumerate((cols, col_alpha)):
            bytes_of(ref, chunks, sent.at[2 + which], recv_c.at[2 * across + which, z]).wait_recv()

    with scope("rdy3"):
        for d in range(3, n_z):
            learn(d)

    early = range(min(CORES, row_size))
    late = range(CORES, row_size)
    if n_y > 1:
        with scope("wy"):
            arrive(my_z, n_y - 1)
        with scope("cy"):
            contribute([(m, k) for m in range(1, n_y) for k in early])
    if row_size > CORES:
        with scope("wrow"):
            for k in late:
                row_arrival(k).wait_recv()
        with scope("crow"):
            for k in late:
                prepare_rows(k)
            contribute([(m, k) for m in range(n_y) for k in late])

    for at in range(1, n_z):
        with scope("wz"):
            arrive(order[at], 1)
            if n_y > 1:
                arrive(order[at], n_y - 1, across=1)
        with scope("cz"):
            contribute(
                [(at * n_y + m, k) for m in range(n_y) for k in range(row_size)],
                last=at == n_z - 1,
            )

    with scope("fold"):
        bytes_of(row_alpha, row_size - 1, sent.at[1], recv_ra.at[0]).wait_recv()
        folded = None
        for k in range(row_size):
            total = acc[k]
            row_scaled = rows[k] * inverse
            first = total[0:16] + total[32:48]
            second = total[16:32] + total[48:64]
            weight = total[64:65] + total[65:66] + total[66:67]
            share = (0.5 * row_alpha[k]) * (
                row_scaled * row_scaled * weight - 2.0 * row_scaled * first + second
            )
            shares[k] = share
            share_sums[k] = weight
            for at in range(0, row_count, 128):
                piece = share[:, at : at + 128]
                folded = piece if folded is None else folded + piece
        gathered = lax.dot_general(
            jnp.ones((8, 128), F32),
            folded,
            (((1,), (1,)), ((), ())),
            precision=lax.Precision.HIGHEST,
            preferred_element_type=F32,
        )
        part[...] = jnp.zeros_like(part)
        part[:, 0:dims] = gathered

    with scope("gst"):
        for place in range(n_all - 1):
            g_copy(place).start()
        for k in row_steps:
            for which in (0, 1):
                term_copy(k, which).start()

    with scope("drain"):
        for which, ref in enumerate((rows, row_alpha)):
            bytes_of(ref, row_size - 1, sent.at[which], recv_r.at[0]).wait_send()
        for which, ref in enumerate((cols, col_alpha)):
            bytes_of(ref, col_size - 1, sent.at[2 + which], recv_r.at[0]).wait_send()

    with scope("twait"):
        for which, ref in enumerate((incoming, incoming_sums)):
            bytes_of(ref, row_size - 1, sent.at[4 + which], recv_t.at[which]).wait_recv()
    with scope("tsum"):
        terms, sums = shares[0], share_sums[0]
        for k in range(1, row_size):
            terms = terms + incoming[k]
            sums = sums + incoming_sums[k]
        terms_ref[...] = terms
        sums_ref[...] = sums
        parts[n_all - 1] = part[0:1]
    with scope("gwait"):
        bytes_of(parts, n_all - 1, sent.at[6], recv_g.at[0]).wait()
    with scope("gsum"):
        grad_ref[...] = (jnp.sum(parts[...], 0) / (row_count * n_all))[:, 0:dims]
        for which, ref in enumerate((shares, share_sums)):
            bytes_of(ref, row_size - 1, sent.at[4 + which], recv_t.at[which]).wait_send()


def settle(terms_in, sums_in, grad_in, terms_out, sums_out, grad_out, sems):
    copies = [
        pltpu.make_async_copy(terms_in, terms_out, sems.at[0]),
        pltpu.make_async_copy(sums_in, sums_out, sems.at[1]),
        pltpu.make_async_copy(grad_in, grad_out, sems.at[2]),
    ]
    for copy in copies:
        copy.start()
    for copy in copies:
        copy.wait()


def on_device(row_size, col_size, x_rows, alpha_rows, x_cols, alpha_cols, lengthscale):
    dims, row_count = x_rows.shape
    col_count = x_cols.shape[1]
    _, _, n_z = layout(row_size, col_size)
    n_all = row_size * col_size
    vmem = pl.BlockSpec(memory_space=pltpu.VMEM)
    anywhere = pl.BlockSpec(memory_space=pl.ANY)
    dma = pltpu.SemaphoreType.DMA
    terms, sums, grad = pl.pallas_call(
        functools.partial(kernel, row_size, col_size),
        out_shape=(
            pltpu.VMEM((dims, row_count), F32),
            pltpu.VMEM((1, row_count), F32),
            pltpu.VMEM((1, dims), F32),
        ),
        in_specs=[pl.BlockSpec(memory_space=pltpu.HBM)] * 5,
        out_specs=(vmem, vmem, vmem),
        scratch_shapes=[
            pltpu.VMEM((1, dims), F32),
            pltpu.VMEM((row_size, dims, row_count), F32),
            pltpu.VMEM((row_size, 1, row_count), F32),
            pltpu.VMEM((col_size, dims, col_count), F32),
            pltpu.VMEM((col_size, 1, col_count), F32),
            pltpu.VMEM((row_size, 112, row_count), BF16),
            pltpu.VMEM((row_size, 80, row_count), F32),
            pltpu.VMEM((LAG + 1, 2 * col_count, row_count), BF16),
            pltpu.VMEM((col_size, 80, col_count), BF16),
            pltpu.VMEM((row_size, dims, row_count), F32),
            pltpu.VMEM((row_size, 1, row_count), F32),
            pltpu.VMEM((row_size, dims, row_count), F32),
            pltpu.VMEM((row_size, 1, row_count), F32),
            pltpu.VMEM((8, 128), F32),
            pltpu.VMEM((n_all, 1, 128), F32),
            dma((5,)),
            pltpu.SemaphoreType.REGULAR((n_z,)),
            dma((7,)),
            dma((row_size,)),
            dma((1,)),
            dma((4, n_z)),
            dma((2,)),
            dma((1,)),
        ],
        compiler_params=pltpu.CompilerParams(
            collective_id=0, has_side_effects=True
        ),
    )(
        x_rows,
        alpha_rows.reshape(1, row_count),
        x_cols,
        alpha_cols.reshape(1, col_count),
        lengthscale.reshape(1, dims),
    )
    terms, sums, grad = pl.pallas_call(
        settle,
        out_shape=[jax.ShapeDtypeStruct(x.shape, x.dtype) for x in (terms, sums, grad)],
        in_specs=[vmem] * 3,
        out_specs=(anywhere, anywhere, anywhere),
        scratch_shapes=[dma((3,))],
        compiler_params=pltpu.CompilerParams(vmem_limit_bytes=16 * 1024 * 1024),
    )(terms, sums, grad)
    return terms, sums.reshape(row_count), grad.reshape(dims)


def solution(mesh):
    return jax.shard_map(
        functools.partial(on_device, mesh.shape["row"], mesh.shape["col"]),
        mesh=mesh,
        in_specs=(
            P(None, ("row", "col")),
            P(("row", "col")),
            P(None, ("col", "row")),
            P(("col", "row")),
            P(),
        ),
        out_specs=(P(None, ("row", "col")), P(("row", "col")), P()),
        check_vma=False,
    )
```

```python
import functools

import jax
import jax.numpy as jnp
from jax import lax
from jax.experimental import pallas as pl
from jax.experimental.pallas import tpu as pltpu
from jax.sharding import PartitionSpec as P

LOG2E = 1.4426950408889634
CORES = 2
MESH = pl.DeviceIdType.MESH
F32 = jnp.float32
BF16 = jnp.bfloat16
scope = jax.named_scope
LAG = 2


def split3(value):
    high = value.astype(BF16)
    rest = value - high.astype(F32)
    mid = rest.astype(BF16)
    low = (rest - mid.astype(F32)).astype(BF16)
    return high, mid, low


def split2(value):
    high = value.astype(BF16)
    mid = (value - high.astype(F32)).astype(BF16)
    return high, mid


def stack_rows(count, rows):
    index = lax.broadcasted_iota(jnp.int32, (16, count), 0)
    out = jnp.zeros((16, count), F32)
    for place, row in enumerate(rows):
        row = row.astype(F32) if hasattr(row, "astype") else row
        out = jnp.where(index == place, row, out)
    return out.astype(BF16)


def layout(row_size, col_size):
    n_x = row_size // CORES
    n_y = n_x if col_size % n_x == 0 else 1
    return n_x, n_y, col_size // n_y


def far_first(row_size, col_size):
    n_x, n_y, n_z = layout(row_size, col_size)
    steps = [
        (dx, core, dz, dy)
        for dx in range(n_x)
        for core in range(CORES)
        for dz in range(n_z)
        for dy in range(n_y)
    ]
    steps.remove((0, 0, 0, 0))

    def hops(step):
        dx, core, dz, dy = step
        return min(dx, n_x - dx) + min(dy, n_y - dy) + min(dz, n_z - dz), core

    return sorted(steps, key=hops, reverse=True)


def kernel(
    row_size,
    col_size,
    xr_hbm,
    ar_hbm,
    xc_hbm,
    ac_hbm,
    ls_hbm,
    terms_ref,
    sums_ref,
    grad_ref,
    ls_ref,
    rows,
    row_alpha,
    cols,
    col_alpha,
    row_aug,
    acc,
    values,
    lefts,
    shares,
    share_sums,
    incoming,
    incoming_sums,
    part,
    parts,
    local,
    ready,
    sent,
    recv_r,
    recv_ra,
    recv_c,
    recv_t,
    recv_g,
):
    _, dims, row_count = rows.shape
    col_count = cols.shape[2]
    n_x, n_y, n_z = layout(row_size, col_size)
    n_all = row_size * col_size
    my_row = lax.axis_index("row")
    my_col = lax.axis_index("col")
    my_x, my_core = my_row // CORES, my_row % CORES
    my_z, my_y = my_col // n_y, my_col % n_y

    def row_peer(k):
        return (
            (my_x + k // CORES) % n_x * CORES + (my_core + k % CORES) % CORES,
            my_col,
        )

    def back(k):
        return (n_x - k // CORES) % n_x * CORES + k % CORES

    low = jnp.minimum(my_z, n_z - 1 - my_z)
    far_sign = jnp.where(2 * my_z < n_z - 1, 1, -1)
    order = [my_z]
    for t in range(1, n_z):
        near = my_z + (1 if t % 2 else -1) * ((t + 1) // 2)
        order.append(jnp.where(t <= 2 * low, near, my_z + far_sign * (t - low)))
    places = [
        [z * n_y + (my_y + m) % n_y for m in range(n_y)] for z in order
    ]
    ordered = [c for line in places for c in line]
    row_steps = list(range(CORES, row_size)) + [1]
    sides = [(1, my_z < n_z - 1), (-1, my_z > 0)]

    def line(z):
        return [(my_row, z * n_y + (my_y + m) % n_y) for m in range(n_y)]

    barrier = pltpu.get_barrier_semaphore()
    for m in range(n_y):
        for sign, there in sides:

            @pl.when(there)
            def _():
                peer = line(my_z + sign)[n_y - 1 - m]
                pl.semaphore_signal(barrier, inc=1, device_id=peer, device_id_type=MESH)

    for peer in line(my_z)[1:]:
        pl.semaphore_signal(barrier, inc=1, device_id=peer, device_id_type=MESH)
    for k in row_steps:
        pl.semaphore_signal(barrier, inc=1, device_id=row_peer(k), device_id_type=MESH)

    loads = [
        pltpu.make_async_copy(xc_hbm, cols.at[my_col], local.at[0]),
        pltpu.make_async_copy(ac_hbm, col_alpha.at[my_col], local.at[1]),
        pltpu.make_async_copy(xr_hbm, rows.at[0], local.at[2]),
        pltpu.make_async_copy(ar_hbm, row_alpha.at[0], local.at[3]),
        pltpu.make_async_copy(ls_hbm, ls_ref, local.at[4]),
    ]
    for copy in loads:
        copy.start()

    def remote(src, dst, send, recv, peer):
        return pltpu.make_async_remote_copy(src, dst, send, recv, peer, MESH)

    def row_copy(k, which):
        ref, there = (rows, row_alpha)[which], back(k)
        return remote(
            ref.at[0],
            ref.at[there],
            sent.at[which],
            recv_ra.at[0] if which else recv_r.at[there],
            row_peer(k),
        )

    def bytes_of(ref, count, send, recv):
        return remote(ref.at[pl.ds(0, count)], ref.at[pl.ds(0, count)], send, recv, row_peer(1))

    def row_arrival(k):
        return remote(rows.at[0], rows.at[k], sent.at[0], recv_r.at[k], row_peer(k))

    def col_copy(peer, which, across):
        ref = (cols, col_alpha)[which]
        return remote(
            ref.at[my_col],
            ref.at[my_col],
            sent.at[2 + which],
            recv_c.at[2 * across + which, my_z],
            peer,
        )

    def send_line(z, first=0):
        for which in (0, 1):
            for m, peer in list(enumerate(line(z)))[first:]:
                col_copy(peer, which, int(m > 0 and not first)).start()

    def learn(d):
        for sign, _ in sides:
            z, other = my_z + sign * d, my_z - sign
            inside = jnp.logical_and(z >= 0, z < n_z)

            @pl.when(inside)
            def _():
                pl.semaphore_wait(ready.at[z], 1)

            @pl.when(jnp.logical_and(inside, jnp.logical_and(other >= 0, other < n_z)))
            def _():
                pl.semaphore_signal(
                    ready.at[z], inc=1, device_id=line(other)[0], device_id_type=MESH
                )

            @pl.when(inside)
            def _():
                send_line(z)

    def term_copy(k, which):
        src, dst = ((shares, incoming), (share_sums, incoming_sums))[which]
        there = back(k)
        return remote(
            src.at[k], dst.at[there], sent.at[4 + which], recv_t.at[which], row_peer(k)
        )

    steps = far_first(row_size, col_size)

    def g_copy(place):
        dx, core, dz, dy = steps[place]
        peer = (
            (my_x + dx) % n_x * CORES + (my_core + core) % CORES,
            (my_z + dz) % n_z * n_y + (my_y + dy) % n_y,
        )
        return remote(
            part.at[pl.ds(0, 1)], parts.at[place], sent.at[6], recv_g.at[0], peer
        )

    with scope("load"):
        for copy in loads:
            copy.wait()

    eye = lax.broadcasted_iota(jnp.int32, (dims, dims), 0) == lax.broadcasted_iota(
        jnp.int32, (dims, dims), 1
    )
    scale = jnp.sum(jnp.where(eye, jnp.broadcast_to(ls_ref[...], (dims, dims)), 0.0), 1, keepdims=True)
    inverse = 1.0 / scale

    def prepare_rows(k):
        row_scaled = rows[k] * inverse
        row_norm = (-0.5 * LOG2E) * jnp.sum(row_scaled * row_scaled, 0, keepdims=True)
        rh, rm, rl = split3(row_scaled * LOG2E)
        row_aug[k] = jnp.concatenate(
            [rh, rh, rh, rm, rm, rl, stack_rows(row_count, (1.0, 1.0, 1.0) + split3(row_norm))], 0
        )

    def operands(c):
        x, alpha = cols[c], col_alpha[c]
        scaled = x * inverse
        norm = (-0.5 * LOG2E) * jnp.sum(scaled * scaled, 0, keepdims=True)
        ch, cm, cl = split3(scaled)
        col_aug = jnp.concatenate(
            [ch, cm, cl, ch, cm, ch, stack_rows(col_count, split3(norm) + (1.0, 1.0, 1.0))], 0
        )
        first = alpha * scaled
        fh, fm = split2(first)
        sh, sm = split2(first * scaled)
        group = stack_rows(col_count, split3(alpha))
        left = jnp.concatenate([fh, sh, fm, sm, group], 0)
        return col_aug, left

    waiting, begun, made = [], set(), set()
    slots = values.shape[0]
    half = col_count // 2
    count = 0

    def high_sums():
        k, place, slot = waiting[0]
        return jnp.dot(lefts[place], values[slot, 0:col_count], preferred_element_type=F32)

    def mid_sums(high):
        k, place, slot = waiting.pop(0)
        left = jnp.concatenate([lefts[place, 0:32], lefts[place, 64:80]], 0)
        mid = jnp.dot(left, values[slot, col_count : 2 * col_count], preferred_element_type=F32)
        parts = (high[0:32] + mid[0:32], high[32:64], high[64:80] + mid[32:48])
        for at, more in zip((0, 32, 64), parts):
            here = slice(at, at + more.shape[0])
            if k in begun:
                acc[k, here] += more
            else:
                acc[k, here] = more
        begun.add(k)
        left_over[k] -= 1
        if not left_over[k]:
            finish(k)

    left_over = {k: col_size for k in range(row_size)}
    folds = []

    def finish(k):
        total = acc[k]
        row_scaled = rows[k] * inverse
        first = total[0:16] + total[32:48]
        second = total[16:32] + total[48:64]
        weight = total[64:65] + total[65:66] + total[66:67]
        share = (0.5 * row_alpha[k]) * (
            row_scaled * row_scaled * weight - 2.0 * row_scaled * first + second
        )
        shares[k] = share
        share_sums[k] = weight
        folds.append(sum(share[:, at : at + 128] for at in range(0, row_count, 128)))

    def exponents_of(aug, k):
        return lax.dot_general(aug, row_aug[k], (((0,), (0,)), ((), ())), preferred_element_type=F32)

    def contribute(pairs, last=False):
        nonlocal count
        pairs = list(pairs)
        while waiting:
            mid_sums(high_sums())
        augs, exponents = {}, {}

        def settle_values(now):
            nonlocal count
            slot = count % slots
            count += 1
            for at, exponent in zip((0, half), exponents.pop(now)):
                high, mid = split2(jnp.exp2(exponent))
                values[slot, at : at + half] = high
                values[slot, col_count + at : col_count + at + half] = mid
            waiting.append((pairs[now][1], pairs[now][0], slot))

        for now, (place, k) in enumerate(pairs):
            if place not in augs:
                augs[place], left = operands(ordered[place])
                if place not in made:
                    lefts[place] = left
                    made.add(place)
            near = exponents_of(augs[place][:, 0:half], k)
            high = high_sums() if waiting else None
            exponents[now] = near, exponents_of(augs[place][:, half:], k)
            if high is not None:
                mid_sums(high)
            if now:
                settle_values(now - 1)
        while waiting:
            mid_sums(high_sums())
        settle_values(len(pairs) - 1)
        while last and waiting:
            mid_sums(high_sums())

    prepare_rows(0)

    with scope("bar"):
        beside = sum(there.astype(jnp.int32) for _, there in sides)
        pl.semaphore_wait(barrier, row_size - 1 + n_y - 1 + beside * n_y)

    with scope("send"):
        @pl.when(jnp.logical_and(sides[0][1], sides[1][1]))
        def _():
            for sign in (1, -1):
                pl.semaphore_signal(
                    ready.at[my_z + sign],
                    inc=1,
                    device_id=line(my_z - sign)[0],
                    device_id_type=MESH,
                )

        send_line(my_z, 1)
        for k in row_steps:
            row_copy(k, 0).start()
        for sign, there in sides:

            @pl.when(there)
            def _():
                send_line(my_z + sign)

        for k in row_steps:
            row_copy(k, 1).start()

    with scope("c00"):
        contribute([(0, 0)], last=True)

    if n_z > 2:
        with scope("rdy2"):
            learn(2)
    with scope("w01"):
        row_arrival(1).wait_recv()
    with scope("c01"):
        prepare_rows(1)
        contribute([(0, 1)], last=True)

    def arrive(z, chunks, across=0):
        for which, ref in enumerate((cols, col_alpha)):
            bytes_of(ref, chunks, sent.at[2 + which], recv_c.at[2 * across + which, z]).wait_recv()

    with scope("rdy3"):
        for d in range(3, n_z):
            learn(d)

    early = range(min(CORES, row_size))
    late = range(CORES, row_size)
    straight = [(at, 0) for at in range(1, n_z)]
    across = [(at, m) for at in range(1, n_z) for m in range(1, n_y)]
    mixed = [one for pair in zip(across, straight[1:]) for one in pair]
    mixed += across[len(straight) - 1 :] if straight else []
    blocks = [straight[:1]] if straight else []
    blocks += [mixed[at : at + 2] for at in range(0, len(mixed), 2)]

    same, other = range(CORES, row_size, CORES), range(CORES + 1, row_size, CORES)
    beside_y = [(0, m) for m in range(1, n_y)]
    with scope("wrow"):
        for k in same:
            row_arrival(k).wait_recv()
        if n_y > 1:
            arrive(my_z, n_y - 1)
    with scope("crow"):
        for k in same:
            prepare_rows(k)
        contribute(
            [(0, k) for k in same] + [(m, k) for _, m in beside_y for k in (*early, *same)]
        )
    with scope("wrow2"):
        for k in other:
            row_arrival(k).wait_recv()
        for k in other:
            prepare_rows(k)
    blocks = [[(0, 0)] + beside_y + sum(blocks[:1], [])] + blocks[1:]

    arrived = set()
    for block in blocks:
        last = block is blocks[-1]
        with scope("wz"):
            for at, m in block:
                if at and (at, m > 0) not in arrived:
                    arrived.add((at, m > 0))
                    arrive(order[at], n_y - 1 if m else 1, across=int(m > 0))
            if last:
                bytes_of(row_alpha, row_size - 1, sent.at[1], recv_ra.at[0]).wait_recv()
        with scope("fold" if last else "cz"):
            pairs = [
                (at * n_y + m, k) for at, m in block for k in (range(row_size) if at else other)
            ]
            if last:
                pairs.sort(key=lambda pair: pair[1])
            contribute(pairs, last=last)
            if last:
                part[...] = jnp.zeros_like(part)
                part[0:1, 0:dims] = jnp.sum(sum(folds).T, 0, keepdims=True)

    with scope("gst"):
        for place in range(n_all - 1):
            g_copy(place).start()
        for k in row_steps:
            for which in (0, 1):
                term_copy(k, which).start()

    with scope("drain"):
        for which, ref in enumerate((rows, row_alpha)):
            bytes_of(ref, row_size - 1, sent.at[which], recv_r.at[0]).wait_send()
        for which, ref in enumerate((cols, col_alpha)):
            bytes_of(ref, col_size - 1, sent.at[2 + which], recv_r.at[0]).wait_send()

    with scope("twait"):
        for which, ref in enumerate((incoming, incoming_sums)):
            bytes_of(ref, row_size - 1, sent.at[4 + which], recv_t.at[which]).wait_recv()
    with scope("tsum"):
        terms, sums = shares[0], share_sums[0]
        for k in range(1, row_size):
            terms = terms + incoming[k]
            sums = sums + incoming_sums[k]
        terms_ref[...] = terms
        sums_ref[...] = sums
        parts[n_all - 1] = part[0:1]
    with scope("gwait"):
        bytes_of(parts, n_all - 1, sent.at[6], recv_g.at[0]).wait()
    with scope("gsum"):
        grad_ref[...] = (jnp.sum(parts[...], 0) / (row_count * n_all))[:, 0:dims]
        for which, ref in enumerate((shares, share_sums)):
            bytes_of(ref, row_size - 1, sent.at[4 + which], recv_t.at[which]).wait_send()


def settle(terms_in, sums_in, grad_in, terms_out, sums_out, grad_out, sems):
    copies = [
        pltpu.make_async_copy(terms_in, terms_out, sems.at[0]),
        pltpu.make_async_copy(sums_in, sums_out, sems.at[1]),
        pltpu.make_async_copy(grad_in, grad_out, sems.at[2]),
    ]
    for copy in copies:
        copy.start()
    for copy in copies:
        copy.wait()


def on_device(row_size, col_size, x_rows, alpha_rows, x_cols, alpha_cols, lengthscale):
    dims, row_count = x_rows.shape
    col_count = x_cols.shape[1]
    _, _, n_z = layout(row_size, col_size)
    n_all = row_size * col_size
    vmem = pl.BlockSpec(memory_space=pltpu.VMEM)
    anywhere = pl.BlockSpec(memory_space=pl.ANY)
    dma = pltpu.SemaphoreType.DMA
    terms, sums, grad = pl.pallas_call(
        functools.partial(kernel, row_size, col_size),
        out_shape=(
            pltpu.VMEM((dims, row_count), F32),
            pltpu.VMEM((1, row_count), F32),
            pltpu.VMEM((1, dims), F32),
        ),
        in_specs=[pl.BlockSpec(memory_space=pltpu.HBM)] * 5,
        out_specs=(vmem, vmem, vmem),
        scratch_shapes=[
            pltpu.VMEM((1, dims), F32),
            pltpu.VMEM((row_size, dims, row_count), F32),
            pltpu.VMEM((row_size, 1, row_count), F32),
            pltpu.VMEM((col_size, dims, col_count), F32),
            pltpu.VMEM((col_size, 1, col_count), F32),
            pltpu.VMEM((row_size, 112, row_count), BF16),
            pltpu.VMEM((row_size, 80, row_count), F32),
            pltpu.VMEM((LAG + 1, 2 * col_count, row_count), BF16),
            pltpu.VMEM((col_size, 80, col_count), BF16),
            pltpu.VMEM((row_size, dims, row_count), F32),
            pltpu.VMEM((row_size, 1, row_count), F32),
            pltpu.VMEM((row_size, dims, row_count), F32),
            pltpu.VMEM((row_size, 1, row_count), F32),
            pltpu.VMEM((8, 128), F32),
            pltpu.VMEM((n_all, 1, 128), F32),
            dma((5,)),
            pltpu.SemaphoreType.REGULAR((n_z,)),
            dma((7,)),
            dma((row_size,)),
            dma((1,)),
            dma((4, n_z)),
            dma((2,)),
            dma((1,)),
        ],
        compiler_params=pltpu.CompilerParams(
            collective_id=0, has_side_effects=True
        ),
    )(
        x_rows,
        alpha_rows.reshape(1, row_count),
        x_cols,
        alpha_cols.reshape(1, col_count),
        lengthscale.reshape(1, dims),
    )
    terms, sums, grad = pl.pallas_call(
        settle,
        out_shape=[jax.ShapeDtypeStruct(x.shape, x.dtype) for x in (terms, sums, grad)],
        in_specs=[vmem] * 3,
        out_specs=(anywhere, anywhere, anywhere),
        scratch_shapes=[dma((3,))],
        compiler_params=pltpu.CompilerParams(vmem_limit_bytes=16 * 1024 * 1024),
    )(terms, sums, grad)
    return terms, sums.reshape(row_count), grad.reshape(dims)


def solution(mesh):
    return jax.shard_map(
        functools.partial(on_device, mesh.shape["row"], mesh.shape["col"]),
        mesh=mesh,
        in_specs=(
            P(None, ("row", "col")),
            P(("row", "col")),
            P(None, ("col", "row")),
            P(("col", "row")),
            P(),
        ),
        out_specs=(P(None, ("row", "col")), P(("row", "col")), P()),
        check_vma=False,
    )
```

```python
import functools

import jax
import jax.numpy as jnp
from jax import lax
from jax.experimental import pallas as pl
from jax.experimental.pallas import tpu as pltpu
from jax.sharding import PartitionSpec as P

LOG2E = 1.4426950408889634
CORES = 2
MESH = pl.DeviceIdType.MESH
F32 = jnp.float32
BF16 = jnp.bfloat16
scope = jax.named_scope
LAG = 2


def split3(value):
    high = value.astype(BF16)
    rest = value - high.astype(F32)
    mid = rest.astype(BF16)
    low = (rest - mid.astype(F32)).astype(BF16)
    return high, mid, low


def split2(value):
    high = value.astype(BF16)
    mid = (value - high.astype(F32)).astype(BF16)
    return high, mid


def stack_rows(count, rows):
    index = lax.broadcasted_iota(jnp.int32, (16, count), 0)
    out = jnp.zeros((16, count), F32)
    for place, row in enumerate(rows):
        row = row.astype(F32) if hasattr(row, "astype") else row
        out = jnp.where(index == place, row, out)
    return out.astype(BF16)


def layout(row_size, col_size):
    n_x = row_size // CORES
    n_y = n_x if col_size % n_x == 0 else 1
    return n_x, n_y, col_size // n_y


def far_first(row_size, col_size):
    n_x, n_y, n_z = layout(row_size, col_size)
    steps = [
        (dx, core, dz, dy)
        for dx in range(n_x)
        for core in range(CORES)
        for dz in range(n_z)
        for dy in range(n_y)
    ]
    steps.remove((0, 0, 0, 0))

    def hops(step):
        dx, core, dz, dy = step
        return min(dx, n_x - dx) + min(dy, n_y - dy) + min(dz, n_z - dz), core

    return sorted(steps, key=hops, reverse=True)


def kernel(
    row_size,
    col_size,
    xr_hbm,
    ar_hbm,
    xc_hbm,
    ac_hbm,
    ls_hbm,
    terms_ref,
    sums_ref,
    grad_ref,
    ls_ref,
    rows,
    row_alpha,
    cols,
    col_alpha,
    row_aug,
    acc,
    values,
    lefts,
    shares,
    share_sums,
    incoming,
    incoming_sums,
    part,
    parts,
    tally,
    local,
    ready,
    sent,
    recv_r,
    recv_c,
    recv_t,
    recv_g,
):
    _, dims, row_count = rows.shape
    col_count = cols.shape[2]
    n_x, n_y, n_z = layout(row_size, col_size)
    n_all = row_size * col_size
    my_row = lax.axis_index("row")
    my_col = lax.axis_index("col")
    my_x, my_core = my_row // CORES, my_row % CORES
    my_z, my_y = my_col // n_y, my_col % n_y

    def row_peer(k):
        return (
            (my_x + k // CORES) % n_x * CORES + (my_core + k % CORES) % CORES,
            my_col,
        )

    def back(k):
        return (n_x - k // CORES) % n_x * CORES + k % CORES

    low = jnp.minimum(my_z, n_z - 1 - my_z)
    far_sign = jnp.where(2 * my_z < n_z - 1, 1, -1)
    order = [my_z]
    for t in range(1, n_z):
        near = my_z + (1 if t % 2 else -1) * ((t + 1) // 2)
        order.append(jnp.where(t <= 2 * low, near, my_z + far_sign * (t - low)))
    places = [
        [z * n_y + (my_y + m) % n_y for m in range(n_y)] for z in order
    ]
    ordered = [c for line in places for c in line]
    row_steps = list(range(CORES, row_size)) + [1]
    sides = [(1, my_z < n_z - 1), (-1, my_z > 0)]

    def line(z):
        return [(my_row, z * n_y + (my_y + m) % n_y) for m in range(n_y)]

    barrier = pltpu.get_barrier_semaphore()
    for m in range(n_y):
        for sign, there in sides:

            @pl.when(there)
            def _():
                peer = line(my_z + sign)[n_y - 1 - m]
                pl.semaphore_signal(barrier, inc=1, device_id=peer, device_id_type=MESH)

    for peer in line(my_z)[1:]:
        pl.semaphore_signal(barrier, inc=1, device_id=peer, device_id_type=MESH)
    for k in row_steps:
        pl.semaphore_signal(barrier, inc=1, device_id=row_peer(k), device_id_type=MESH)

    loads = [
        pltpu.make_async_copy(xc_hbm, cols.at[my_col], local.at[0]),
        pltpu.make_async_copy(ac_hbm, col_alpha.at[my_col], local.at[1]),
        pltpu.make_async_copy(xr_hbm, rows.at[0], local.at[2]),
        pltpu.make_async_copy(ar_hbm, row_alpha.at[0], local.at[3]),
        pltpu.make_async_copy(ls_hbm, ls_ref, local.at[4]),
    ]
    for copy in loads:
        copy.start()

    def remote(src, dst, send, recv, peer):
        return pltpu.make_async_remote_copy(src, dst, send, recv, peer, MESH)

    def row_copy(k, which):
        ref, there = (rows, row_alpha)[which], back(k)
        return remote(
            ref.at[0],
            ref.at[there],
            sent.at[0],
            recv_r.at[there],
            row_peer(k),
        )

    def bytes_of(blocks, count, send, recv):
        size = pl.ds(0, blocks * (dims + 1) * count // 128)
        return remote(tally.at[size], tally.at[size], send, recv, row_peer(1))

    def row_arrival(k):
        bytes_of(1, row_count, sent.at[0], recv_r.at[k]).wait_recv()

    def col_copy(peer, which, across):
        ref = (cols, col_alpha)[which]
        return remote(
            ref.at[my_col],
            ref.at[my_col],
            sent.at[1],
            recv_c.at[across, my_z],
            peer,
        )

    def send_line(z, first=0):
        for which in (0, 1):
            for m, peer in list(enumerate(line(z)))[first:]:
                col_copy(peer, which, int(m > 0 and not first)).start()

    def learn(d):
        for sign, _ in sides:
            z, other = my_z + sign * d, my_z - sign
            inside = jnp.logical_and(z >= 0, z < n_z)

            @pl.when(inside)
            def _():
                pl.semaphore_wait(ready.at[z], 1)

            @pl.when(jnp.logical_and(inside, jnp.logical_and(other >= 0, other < n_z)))
            def _():
                pl.semaphore_signal(
                    ready.at[z], inc=1, device_id=line(other)[0], device_id_type=MESH
                )

            @pl.when(inside)
            def _():
                send_line(z)

    def term_copy(k, which):
        src, dst = ((shares, incoming), (share_sums, incoming_sums))[which]
        there = back(k)
        return remote(
            src.at[k], dst.at[there], sent.at[2], recv_t.at[0], row_peer(k)
        )

    steps = far_first(row_size, col_size)

    def g_copy(place):
        dx, core, dz, dy = steps[place]
        peer = (
            (my_x + dx) % n_x * CORES + (my_core + core) % CORES,
            (my_z + dz) % n_z * n_y + (my_y + dy) % n_y,
        )
        return remote(
            part.at[pl.ds(0, 1)], parts.at[place], sent.at[3], recv_g.at[0], peer
        )

    with scope("load"):
        for copy in loads:
            copy.wait()

    eye = lax.broadcasted_iota(jnp.int32, (dims, dims), 0) == lax.broadcasted_iota(
        jnp.int32, (dims, dims), 1
    )
    scale = jnp.sum(jnp.where(eye, jnp.broadcast_to(ls_ref[...], (dims, dims)), 0.0), 1, keepdims=True)
    inverse = 1.0 / scale

    def prepare_rows(k):
        row_scaled = rows[k] * inverse
        row_norm = (-0.5 * LOG2E) * jnp.sum(row_scaled * row_scaled, 0, keepdims=True)
        rh, rm, rl = split3(row_scaled * LOG2E)
        row_aug[k] = jnp.concatenate(
            [rh, rh, rh, rm, rm, rl, stack_rows(row_count, (1.0, 1.0, 1.0) + split3(row_norm))], 0
        )

    def operands(c):
        x, alpha = cols[c], col_alpha[c]
        scaled = x * inverse
        norm = (-0.5 * LOG2E) * jnp.sum(scaled * scaled, 0, keepdims=True)
        ch, cm, cl = split3(scaled)
        col_aug = jnp.concatenate(
            [ch, cm, cl, ch, cm, ch, stack_rows(col_count, split3(norm) + (1.0, 1.0, 1.0))], 0
        )
        first = alpha * scaled
        fh, fm = split2(first)
        sh, sm = split2(first * scaled)
        group = stack_rows(col_count, split3(alpha))
        left = jnp.concatenate([fh, sh, fm, sm, group], 0)
        return col_aug, left

    waiting, begun, made = [], set(), set()
    slots = values.shape[0]
    half = col_count // 2
    count = 0

    def high_sums():
        k, place, slot = waiting[0]
        return jnp.dot(lefts[place], values[slot, 0:col_count], preferred_element_type=F32)

    def mid_sums(high):
        k, place, slot = waiting.pop(0)
        left = jnp.concatenate([lefts[place, 0:32], lefts[place, 64:80]], 0)
        mid = jnp.dot(left, values[slot, col_count : 2 * col_count], preferred_element_type=F32)
        parts = (high[0:32] + mid[0:32], high[32:64], high[64:80] + mid[32:48])
        for at, more in zip((0, 32, 64), parts):
            here = slice(at, at + more.shape[0])
            if k in begun:
                acc[k, here] += more
            else:
                acc[k, here] = more
        begun.add(k)
        left_over[k] -= 1
        if not left_over[k]:
            finish(k)

    left_over = {k: col_size for k in range(row_size)}
    folds = []

    def finish(k):
        total = acc[k]
        row_scaled = rows[k] * inverse
        first = total[0:16] + total[32:48]
        second = total[16:32] + total[48:64]
        weight = total[64:65] + total[65:66] + total[66:67]
        share = (0.5 * row_alpha[k]) * (
            row_scaled * row_scaled * weight - 2.0 * row_scaled * first + second
        )
        shares[k] = share
        share_sums[k] = weight
        folds.append(sum(share[:, at : at + 128] for at in range(0, row_count, 128)))

    def exponents_of(aug, k):
        return lax.dot_general(aug, row_aug[k], (((0,), (0,)), ((), ())), preferred_element_type=F32)

    def contribute(pairs, last=False):
        nonlocal count
        pairs = list(pairs)
        while waiting:
            mid_sums(high_sums())
        augs, exponents = {}, {}

        def settle_values(now):
            nonlocal count
            slot = count % slots
            count += 1
            for at, exponent in zip((0, half), exponents.pop(now)):
                high, mid = split2(jnp.exp2(exponent))
                values[slot, at : at + half] = high
                values[slot, col_count + at : col_count + at + half] = mid
            waiting.append((pairs[now][1], pairs[now][0], slot))

        for now, (place, k) in enumerate(pairs):
            if place not in augs:
                augs[place], left = operands(ordered[place])
                if place not in made:
                    lefts[place] = left
                    made.add(place)
            near = exponents_of(augs[place][:, 0:half], k)
            high = high_sums() if waiting else None
            exponents[now] = near, exponents_of(augs[place][:, half:], k)
            if high is not None:
                mid_sums(high)
            if now:
                settle_values(now - 1)
        while waiting:
            mid_sums(high_sums())
        settle_values(len(pairs) - 1)
        while last and waiting:
            mid_sums(high_sums())

    prepare_rows(0)

    with scope("bar"):
        beside = sum(there.astype(jnp.int32) for _, there in sides)
        pl.semaphore_wait(barrier, row_size - 1 + n_y - 1 + beside * n_y)

    with scope("send"):
        @pl.when(jnp.logical_and(sides[0][1], sides[1][1]))
        def _():
            for sign in (1, -1):
                pl.semaphore_signal(
                    ready.at[my_z + sign],
                    inc=1,
                    device_id=line(my_z - sign)[0],
                    device_id_type=MESH,
                )

        send_line(my_z, 1)
        for k in row_steps:
            row_copy(k, 0).start()
            row_copy(k, 1).start()
        for sign, there in sides:

            @pl.when(there)
            def _():
                send_line(my_z + sign)

    with scope("c00"):
        contribute([(0, 0)], last=True)

    if n_z > 2:
        with scope("rdy2"):
            learn(2)
    with scope("w01"):
        row_arrival(1)
    with scope("c01"):
        prepare_rows(1)
        contribute([(0, 1)], last=True)

    def arrive(z, chunks, across=0):
        bytes_of(chunks, col_count, sent.at[1], recv_c.at[across, z]).wait_recv()

    with scope("rdy3"):
        for d in range(3, n_z):
            learn(d)

    early = range(min(CORES, row_size))
    late = range(CORES, row_size)
    straight = [(at, 0) for at in range(1, n_z)]
    across = [(at, m) for at in range(1, n_z) for m in range(1, n_y)]
    mixed = [one for pair in zip(across, straight[1:]) for one in pair]
    mixed += across[len(straight) - 1 :] if straight else []
    blocks = [straight[:1]] if straight else []
    blocks += [mixed[at : at + 2] for at in range(0, len(mixed), 2)]

    same, other = range(CORES, row_size, CORES), range(CORES + 1, row_size, CORES)
    beside_y = [(0, m) for m in range(1, n_y)]
    with scope("wrow"):
        for k in same:
            row_arrival(k)
        if n_y > 1:
            arrive(my_z, n_y - 1)
    with scope("crow"):
        for k in same:
            prepare_rows(k)
        contribute(
            [(0, k) for k in same] + [(m, k) for _, m in beside_y for k in (*early, *same)]
        )
    with scope("wrow2"):
        for k in other:
            row_arrival(k)
        for k in other:
            prepare_rows(k)
    blocks = [[(0, 0)] + beside_y + sum(blocks[:1], [])] + blocks[1:]

    arrived = set()
    for block in blocks:
        last = block is blocks[-1]
        with scope("wz"):
            for at, m in block:
                if at and (at, m > 0) not in arrived:
                    arrived.add((at, m > 0))
                    arrive(order[at], n_y - 1 if m else 1, across=int(m > 0))
        with scope("fold" if last else "cz"):
            pairs = [
                (at * n_y + m, k) for at, m in block for k in (range(row_size) if at else other)
            ]
            if last:
                pairs.sort(key=lambda pair: pair[1])
            contribute(pairs, last=last)
            if last:
                part[...] = jnp.zeros_like(part)
                part[0:1, 0:dims] = jnp.sum(sum(folds).T, 0, keepdims=True)

    with scope("gst"):
        for place in range(n_all - 1):
            g_copy(place).start()
        for k in row_steps:
            for which in (0, 1):
                term_copy(k, which).start()

    with scope("drain"):
        bytes_of(row_size - 1, row_count, sent.at[0], recv_r.at[0]).wait_send()
        bytes_of(col_size - 1, col_count, sent.at[1], recv_r.at[0]).wait_send()

    with scope("twait"):
        bytes_of(row_size - 1, row_count, sent.at[2], recv_t.at[0]).wait_recv()
    with scope("tsum"):
        terms, sums = shares[0], share_sums[0]
        for k in range(1, row_size):
            terms = terms + incoming[k]
            sums = sums + incoming_sums[k]
        terms_ref[...] = terms
        sums_ref[...] = sums
        parts[n_all - 1] = part[0:1]
    with scope("gwait"):
        remote(
            parts.at[pl.ds(0, n_all - 1)],
            parts.at[pl.ds(0, n_all - 1)],
            sent.at[3],
            recv_g.at[0],
            row_peer(1),
        ).wait()
    with scope("gsum"):
        grad_ref[...] = (jnp.sum(parts[...], 0) / (row_count * n_all))[:, 0:dims]
        bytes_of(row_size - 1, row_count, sent.at[2], recv_t.at[0]).wait_send()


def settle(terms_in, sums_in, grad_in, terms_out, sums_out, grad_out, sems):
    copies = [
        pltpu.make_async_copy(terms_in, terms_out, sems.at[0]),
        pltpu.make_async_copy(sums_in, sums_out, sems.at[1]),
        pltpu.make_async_copy(grad_in, grad_out, sems.at[2]),
    ]
    for copy in copies:
        copy.start()
    for copy in copies:
        copy.wait()


def on_device(row_size, col_size, x_rows, alpha_rows, x_cols, alpha_cols, lengthscale):
    dims, row_count = x_rows.shape
    col_count = x_cols.shape[1]
    _, _, n_z = layout(row_size, col_size)
    n_all = row_size * col_size
    most = max(row_size * row_count, col_size * col_count)
    vmem = pl.BlockSpec(memory_space=pltpu.VMEM)
    anywhere = pl.BlockSpec(memory_space=pl.ANY)
    dma = pltpu.SemaphoreType.DMA
    terms, sums, grad = pl.pallas_call(
        functools.partial(kernel, row_size, col_size),
        out_shape=(
            pltpu.VMEM((dims, row_count), F32),
            pltpu.VMEM((1, row_count), F32),
            pltpu.VMEM((1, dims), F32),
        ),
        in_specs=[pl.BlockSpec(memory_space=pltpu.HBM)] * 5,
        out_specs=(vmem, vmem, vmem),
        scratch_shapes=[
            pltpu.VMEM((1, dims), F32),
            pltpu.VMEM((row_size, dims, row_count), F32),
            pltpu.VMEM((row_size, 1, row_count), F32),
            pltpu.VMEM((col_size, dims, col_count), F32),
            pltpu.VMEM((col_size, 1, col_count), F32),
            pltpu.VMEM((row_size, 112, row_count), BF16),
            pltpu.VMEM((row_size, 80, row_count), F32),
            pltpu.VMEM((LAG + 1, 2 * col_count, row_count), BF16),
            pltpu.VMEM((col_size, 80, col_count), BF16),
            pltpu.VMEM((row_size, dims, row_count), F32),
            pltpu.VMEM((row_size, 1, row_count), F32),
            pltpu.VMEM((row_size, dims, row_count), F32),
            pltpu.VMEM((row_size, 1, row_count), F32),
            pltpu.VMEM((8, 128), F32),
            pltpu.VMEM((n_all, 1, 128), F32),
            pltpu.VMEM((most * (dims + 1) // 128, 1, 128), F32),
            dma((5,)),
            pltpu.SemaphoreType.REGULAR((n_z,)),
            dma((4,)),
            dma((row_size,)),
            dma((2, n_z)),
            dma((1,)),
            dma((1,)),
        ],
        compiler_params=pltpu.CompilerParams(
            collective_id=0, has_side_effects=True
        ),
    )(
        x_rows,
        alpha_rows.reshape(1, row_count),
        x_cols,
        alpha_cols.reshape(1, col_count),
        lengthscale.reshape(1, dims),
    )
    terms, sums, grad = pl.pallas_call(
        settle,
        out_shape=[jax.ShapeDtypeStruct(x.shape, x.dtype) for x in (terms, sums, grad)],
        in_specs=[vmem] * 3,
        out_specs=(anywhere, anywhere, anywhere),
        scratch_shapes=[dma((3,))],
        compiler_params=pltpu.CompilerParams(vmem_limit_bytes=16 * 1024 * 1024),
    )(terms, sums, grad)
    return terms, sums.reshape(row_count), grad.reshape(dims)


def solution(mesh):
    return jax.shard_map(
        functools.partial(on_device, mesh.shape["row"], mesh.shape["col"]),
        mesh=mesh,
        in_specs=(
            P(None, ("row", "col")),
            P(("row", "col")),
            P(None, ("col", "row")),
            P(("col", "row")),
            P(),
        ),
        out_specs=(P(None, ("row", "col")), P(("row", "col")), P()),
        check_vma=False,
    )
```
